32 devices in a mesh: owner: 8 (over z, y), rows: 4 (over x, core).
Axes of the slice: x: 2, y: 2, z: 4, core: 2. Of those that a mesh axis runs over, the one named last changes fastest.
Arguments:
- master_down: float32 [16, 6400, 4096], P('owner', None, 'rows'), may hold values from -0.109375 to 0.109375
- router_weight: float32 [4096, 16], P('rows', 'owner'), may hold values from -0.09375 to 0.09375
- router_gain: float32 [4096], P('rows'), may hold values from 0.25 to 1.75
Outputs:
- final_down: bfloat16 [16, 6400, 4096], P('owner', 'rows')
- scale_down: float32 [16, 6400], P('owner', 'rows')
- serve_router: bfloat16 [4096, 16], replicated
The draws below stay inside these ranges and needn't reach their ends.
All inputs are finite; a program needn't handle non-finite values. Where the reference program divides by a largest or mean magnitude, that divisor is 1e-20 or more.
Results may differ from the reference program's by a relative error of at most 0.001.
Values may be sent and summed in bfloat16 or wider, within the bound.
A program may use at most 192 MiB of HBM per device.

```python
import jax
import jax.numpy as jnp

EXPERTS = 16
D_MODEL = 4096
D_EXPERT = 6400


def with_spikes(entries, rng, source, target, blocks, factor):
    owner, partner = [(jnp.arange(entries.shape[position]) // (entries.shape[position] // blocks)).reshape([-1 if axis == position else 1 for axis in range(entries.ndim)]) for position in (source, target)]
    chosen = jax.random.permutation(rng, blocks)[partner]
    strong = (owner == chosen) | (owner == (partner + blocks // 2) % blocks)
    return jnp.where(strong, factor * entries, entries)


def level_of(key, dims, cuts, low, largest):
    def one(axis_at, shards_of):
        heights = jax.random.uniform(jax.random.fold_in(jax.random.fold_in(key, 6), axis_at), (shards_of,), jnp.float32, low / len(cuts), largest / len(cuts))
        return jnp.repeat(jnp.exp(heights), dims[axis_at] // shards_of).reshape((-1,) + (1,) * (len(dims) - axis_at - 1))

    level = one(*cuts[0])
    for cut in cuts[1:]:
        level = level * one(*cut)
    return level


def gaussian(own_key, extent, deviation, bound, shards=(), dtype=jnp.bfloat16):
    drawn = deviation * jax.random.normal(own_key, extent, jnp.float32)
    if shards:
        drawn = drawn * level_of(own_key, extent, shards, -0.22, 0.18)
    return jnp.clip(drawn, -bound, bound).astype(dtype)


def heavy_noise(rng, dims, spread, bound, split, heavy, held_as=jnp.bfloat16):
    entries = spread * jax.random.normal(rng, dims, jnp.float32)
    if split:
        entries = entries * level_of(rng, dims, split, -0.22, 0.18)
    return jnp.clip(with_spikes(entries, jax.random.fold_in(rng, 3), *heavy), -bound, bound).astype(held_as)


def setup_inputs(seed: int = 0) -> dict:
    key_list = jax.random.split(jax.random.key(seed), 4)
    return {
        "master_down": heavy_noise(key_list[0], (EXPERTS, D_EXPERT, D_MODEL), D_EXPERT ** -0.5, 0.109375, ((0, 8), (2, 4)), (2, 1, 4, 2.0), jnp.float32),
        "router_weight": gaussian(key_list[1], (D_MODEL, EXPERTS), D_MODEL ** -0.5, 0.09375, ((0, 4), (1, 8)), jnp.float32),
        "router_gain": jnp.clip(1.0 + 0.15 * jax.random.normal(key_list[2], (D_MODEL,), jnp.float32), 0.25, 1.75),
    }


def reference(master_down, router_weight, router_gain):
    scale_down = jnp.sum(jnp.abs(master_down), axis=2) / D_MODEL
    final_down = (master_down / jnp.expand_dims(scale_down, 2)).astype(jnp.bfloat16)
    serve_router = (router_weight * router_gain[:, None]).astype(jnp.bfloat16)
    return final_down, scale_down, serve_router
```

```python
import functools

import jax
import jax.numpy as jnp
from jax import lax
from jax.experimental import pallas as pl
from jax.experimental.pallas import tpu as pltpu
from jax.sharding import PartitionSpec as P

LANES = 128
SLOTS = 3


def rows_per_block(quota, n):
    fits = [r for r in range(16, quota + 1, 16) if quota % r == 0 and (n * r) % LANES == 0]
    small = [r for r in fits if r * n <= 1280 and r <= 160]
    return max(small) if small else (min(fits) if fits else quota)


def kernel(n, owners, steps, first, per, x_ref, weight_ref, gain_ref, out_ref, scale_ref, router_ref, fbuf, nbuf, acc, mine, peers,
           strip, load_sem, send_sem, recv_sem, sum_send, sum_recv, strip_send, strip_recv,
           router_send, router_recv):
    me = lax.axis_index("rows")
    home = lax.axis_index("owner")
    rows, width = fbuf.shape[2], fbuf.shape[3]
    groups = width // LANES

    barrier = pltpu.get_barrier_semaphore()
    for d in range(1, n):
        pl.semaphore_signal(
            barrier, inc=1, device_id={"rows": lax.rem(me + d, n)},
            device_id_type=pl.DeviceIdType.MESH,
        )
    for d in range(1, owners):
        pl.semaphore_signal(
            barrier, inc=1, device_id={"owner": lax.rem(home + d, owners)},
            device_id_type=pl.DeviceIdType.MESH,
        )
    strip[me] = (weight_ref[...] * gain_ref[...]).astype(jnp.bfloat16)

    def row_strip(d):
        return pltpu.make_async_remote_copy(
            src_ref=strip.at[me],
            dst_ref=strip.at[me],
            send_sem=strip_send.at[d - 1],
            recv_sem=strip_recv.at[d - 1],
            device_id={"rows": lax.rem(me + d, n)},
            device_id_type=pl.DeviceIdType.MESH,
        )

    def owner_strips(d):
        return pltpu.make_async_remote_copy(
            src_ref=strip,
            dst_ref=router_ref.at[home],
            send_sem=router_send.at[d - 1],
            recv_sem=router_recv.at[d - 1],
            device_id={"owner": lax.rem(home + d, owners)},
            device_id_type=pl.DeviceIdType.MESH,
        )

    def load(t):
        slot = t % SLOTS
        return pltpu.make_async_copy(x_ref.at[t // per, :, t % per], fbuf.at[slot], load_sem.at[slot])

    def prefetch(lo, hi):
        for t in range(lo, min(lo + SLOTS - 1, hi)):
            load(t).start()

    def stream(lo, hi, body):
        def step(t, carry):
            @pl.when(t + SLOTS - 1 < hi)
            def _():
                load(t + SLOTS - 1).start()

            load(t).wait()
            body(t, t % SLOTS)
            return carry

        lax.fori_loop(lo, hi, step, 0)

    def add_up(t, slot):
        for j in range(n):
            part = jnp.abs(fbuf[slot, j, :, :LANES])
            for g in range(1, groups):
                part = part + jnp.abs(fbuf[slot, j, :, g * LANES:(g + 1) * LANES])
            acc[j * rows:(j + 1) * rows, :] = part
        mine[t] = jnp.sum(acc[...].T, axis=0, keepdims=True)

    def exchange(turn, lo, hi):
        return [
            pltpu.make_async_remote_copy(
                src_ref=mine.at[pl.ds(lo, hi - lo)],
                dst_ref=peers.at[d - 1, pl.ds(lo, hi - lo)],
                send_sem=sum_send.at[turn, d - 1],
                recv_sem=sum_recv.at[turn, d - 1],
                device_id={"rows": lax.rem(me + d, n)},
                device_id_type=pl.DeviceIdType.MESH,
            )
            for d in range(1, n)
        ]

    def block(t, d):
        there = lax.rem(me + d, n)
        return pltpu.make_async_remote_copy(
            src_ref=nbuf.at[t, d - 1],
            dst_ref=out_ref.at[t // per, pl.ds(pl.multiple_of((t % per) * rows, rows), rows),
                               pl.ds(pl.multiple_of(me * width, width), width)],
            send_sem=send_sem.at[d - 1, t],
            recv_sem=recv_sem.at[d - 1, t],
            device_id={"rows": there},
            device_id_type=pl.DeviceIdType.MESH,
        )

    def send(t):
        for d in range(1, n):
            block(t, d).start()

    def narrow(t):
        total = mine[t]
        for d in range(1, n):
            total = total + peers[d - 1, t]
        scale = total / (n * width)
        scale_ref[pl.ds(t, 1), :] = scale
        acc[...] = jnp.broadcast_to(1.0 / scale, (LANES, n * rows)).T

    def scale_and_send(lo):
        def body(t, slot):
            narrow(t)
            for d in range(n):
                j = lax.rem(me + d, n)
                inverse = acc[pl.ds(pl.multiple_of(j * rows, rows), rows), :]
                for g in range(groups):
                    cut = slice(g * LANES, (g + 1) * LANES)
                    value = (fbuf[slot, j, :, cut] * inverse).astype(jnp.bfloat16)
                    if d:
                        nbuf[t, d - 1, :, cut] = value
                    else:
                        out_ref[t // per, pl.ds(pl.multiple_of((t % per) * rows, rows), rows),
                                pl.ds(pl.multiple_of(me * width + g * LANES, LANES), LANES)] = value

            @pl.when(t > lo)
            def _():
                send(t - 1)

        return body

    prefetch(0, first)
    stream(0, first, add_up)
    prefetch(0, first)
    pl.semaphore_wait(barrier, n - 1 + owners - 1)
    sums = exchange(0, 0, first)
    for copy in sums:
        copy.start()
    for d in range(1, n):
        row_strip(d).start()
    for copy in sums:
        copy.wait()
    stream(0, first, scale_and_send(0))
    for d in range(1, n):
        row_strip(d).wait()
    for d in range(1, owners):
        owner_strips(d).start()
    router_ref[home] = strip[...]
    if first < steps:
        prefetch(first, steps)
        stream(first, steps, add_up)
        prefetch(first, steps)
        sums = exchange(1, first, steps)
        for copy in sums:
            copy.start()
        send(first - 1)
        for copy in sums:
            copy.wait()
        stream(first, steps, scale_and_send(first))
    send(steps - 1)

    def finish(t, carry):
        for d in range(1, n):
            block(t, d).wait()
        return carry

    lax.fori_loop(0, steps, finish, 0)
    for d in range(1, owners):
        owner_strips(d).wait()


CUTS = 10


def store(x_ref, out_ref, sem):
    height = x_ref.shape[1] // CUTS

    def piece(t):
        return pltpu.make_async_copy(
            x_ref.at[:, pl.ds(t * height, height)], out_ref.at[:, pl.ds(t * height, height)], sem.at[t]
        )

    for t in range(CUTS):
        piece(t).start()
    for t in range(CUTS):
        piece(t).wait()


def per_device(n, owners, master_down, router_weight, router_gain):
    experts, height, width = master_down.shape
    quota = height // n
    rows = rows_per_block(quota, n)
    per = quota // rows
    steps = experts * per
    first = min(max(3, -(-steps // 8)), steps)
    cut = n * rows
    depth, mine = router_weight.shape
    final_down, scales, strips = pl.pallas_call(
        functools.partial(kernel, n, owners, steps, first, per),
        out_shape=(
            pltpu.VMEM((experts, quota, n * width), jnp.bfloat16),
            jax.ShapeDtypeStruct((steps, cut), jnp.float32),
            jax.ShapeDtypeStruct((owners, n, mine, depth), jnp.bfloat16),
        ),
        in_specs=[
            pl.BlockSpec(memory_space=pl.ANY),
            pl.BlockSpec(memory_space=pltpu.VMEM),
            pl.BlockSpec(memory_space=pltpu.VMEM),
        ],
        out_specs=(
            pl.BlockSpec(memory_space=pltpu.VMEM),
            pl.BlockSpec(memory_space=pltpu.VMEM),
            pl.BlockSpec(memory_space=pltpu.VMEM),
        ),
        scratch_shapes=[
            pltpu.VMEM((SLOTS, n, rows, width), jnp.float32),
            pltpu.VMEM((steps, n - 1, rows, width), jnp.bfloat16),
            pltpu.VMEM((cut, LANES), jnp.float32),
            pltpu.VMEM((steps, 1, cut), jnp.float32),
            pltpu.VMEM((n - 1, steps, 1, cut), jnp.float32),
            pltpu.VMEM((n, mine, depth), jnp.bfloat16),
            pltpu.SemaphoreType.DMA((SLOTS,)),
            pltpu.SemaphoreType.DMA((n - 1, steps)),
            pltpu.SemaphoreType.DMA((n - 1, steps)),
            pltpu.SemaphoreType.DMA((2, n - 1)),
            pltpu.SemaphoreType.DMA((2, n - 1)),
            pltpu.SemaphoreType.DMA((n - 1,)),
            pltpu.SemaphoreType.DMA((n - 1,)),
            pltpu.SemaphoreType.DMA((owners - 1,)),
            pltpu.SemaphoreType.DMA((owners - 1,)),
        ],
        compiler_params=pltpu.CompilerParams(
            collective_id=0, has_side_effects=True, vmem_limit_bytes=29 * 1024 * 1024,
        ),
    )(master_down.reshape(experts, n, per, rows, width), router_weight.T, router_gain[None, :])
    final_down = pl.pallas_call(
        store,
        out_shape=jax.ShapeDtypeStruct(final_down.shape, final_down.dtype),
        in_specs=[pl.BlockSpec(memory_space=pltpu.VMEM)],
        out_specs=pl.BlockSpec(memory_space=pl.ANY),
        scratch_shapes=[pltpu.SemaphoreType.DMA((CUTS,))],
        compiler_params=pltpu.CompilerParams(vmem_limit_bytes=1024 * 1024),
    )(final_down)
    final_down, scales, strips = lax.optimization_barrier((final_down, scales, strips))
    by_device = scales.reshape(experts, per, n, rows)
    scale_down = lax.dynamic_index_in_dim(by_device, lax.axis_index("rows"), axis=2, keepdims=False)
    scale_down = scale_down.reshape(experts, quota)

    serve_router = strips.transpose(0, 2, 1, 3).reshape(owners * mine, n * depth).T
    return (final_down, scale_down, serve_router)


def solution(mesh):
    return jax.shard_map(
        functools.partial(per_device, mesh.shape["rows"], mesh.shape["owner"]),
        mesh=mesh,
        in_specs=(P("owner", None, "rows"), P("rows", "owner"), P("rows")),
        out_specs=(P("owner", "rows", None), P("owner", "rows"), P()),
        check_vma=False,
    )
```

```python
import functools

import jax
import jax.numpy as jnp
from jax import lax
from jax.experimental import pallas as pl
from jax.experimental.pallas import tpu as pltpu
from jax.sharding import PartitionSpec as P


LANES = 128
MIB = 1024 * 1024
ANY = pl.BlockSpec(memory_space=pl.ANY)
VMEM = pl.BlockSpec(memory_space=pltpu.VMEM)
STAGES = ((1, 3, 5), (9, 14), (22, 30, 38, 45, 49, 50))


def block_rows(quota, count):
    fits = [r for r in (32, 16, 8) if quota % r == 0 and (count * r) % LANES == 0]
    return fits[0] if fits else quota


def partner(me, d, n):
    return me ^ d if n & (n - 1) == 0 else lax.rem(me + d, n)


def source(me, d, n):
    return me ^ d if n & (n - 1) == 0 else lax.rem(me + n - d, n)


def pairs(d, n):
    return [(i, i ^ d if n & (n - 1) == 0 else (i + d) % n) for i in range(n)]


def add_block(x, acc, rows):
    experts, n, _, width = x.shape
    for e in range(experts):
        for j in range(n):
            part = jnp.abs(x[e, j, :, :LANES])
            for g in range(1, width // LANES):
                part = part + jnp.abs(x[e, j, :, g * LANES:(g + 1) * LANES])
            at = (e * n + j) * rows
            acc[at:at + rows, :] = part
    return jnp.sum(acc[...].T, axis=0, keepdims=True)


def scale_block(x, total, acc, put, me, n, rows):
    experts, _, _, width = x.shape
    acc[...] = jnp.broadcast_to(1.0 / total, (LANES, acc.shape[0])).T
    for d in range(n):
        j = partner(me, d, n)
        for e in range(experts):
            inverse = acc[pl.ds(pl.multiple_of((e * n + j) * rows, rows), rows), :]
            for g in range(width // LANES):
                cut = slice(g * LANES, (g + 1) * LANES)
                put(d, e, cut, (x[e, j, :, cut] * inverse).astype(jnp.bfloat16))


def head(n, rows, x_ref, weight_ref, gain_ref, *refs):
    sent, (own_ref, mine, peers, scale_ref, strip) = refs[:n - 1], refs[n - 1:n + 4]
    (xbuf, acc, weight, gain, load_sem, small_sem, sum_send, sum_recv, strip_send, strip_recv) = refs[n + 4:]
    me = lax.axis_index("rows")
    blocks, width = xbuf.shape[0], xbuf.shape[-1]

    def load(b):
        return pltpu.make_async_copy(x_ref.at[:, :, pl.ds(b * rows, rows)], xbuf.at[b], load_sem.at[b])

    for b in range(blocks):
        load(b).start()
    smalls = [pltpu.make_async_copy(weight_ref, weight, small_sem.at[0]),
              pltpu.make_async_copy(gain_ref, gain, small_sem.at[1])]
    for copy in smalls:
        copy.start()
    barrier = pltpu.get_barrier_semaphore()
    for d in range(1, n):
        pl.semaphore_signal(barrier, inc=1, device_id={"rows": partner(me, d, n)},
                            device_id_type=pl.DeviceIdType.MESH)

    def remote(src, dst, send, recv, d):
        return pltpu.make_async_remote_copy(
            src_ref=src, dst_ref=dst, send_sem=send, recv_sem=recv,
            device_id={"rows": partner(me, d, n)}, device_id_type=pl.DeviceIdType.MESH)

    def sums(turn, lo, hi):
        return [
            remote(mine.at[pl.ds(lo, hi - lo)], peers.at[d - 1, pl.ds(lo, hi - lo)],
                   sum_send.at[turn, d - 1], sum_recv.at[turn, d - 1], d)
            for d in range(1, n)
        ]

    load(0).wait()
    mine[0] = add_block(xbuf.at[0], acc, rows)
    pl.semaphore_wait(barrier, n - 1)
    turns = [sums(0, 0, 1)] + ([sums(1, 1, blocks)] if blocks > 1 else [])
    for copy in turns[0]:
        copy.start()
    for copy in smalls:
        copy.wait()
    strip[me] = (weight[...] * gain[...]).astype(jnp.bfloat16)
    strips = [remote(strip.at[me], strip.at[me], strip_send.at[d - 1], strip_recv.at[d - 1], d)
              for d in range(1, n)]
    for copy in strips:
        copy.start()
    for b in range(1, blocks):
        load(b).wait()
        mine[b] = add_block(xbuf.at[b], acc, rows)
    for turn in turns[1:]:
        for copy in turn:
            copy.start()
    for copy in turns[0]:
        copy.wait()
    total = mine[0]
    for d in range(1, n):
        total = total + peers[d - 1, 0]
    scale = total / (n * width)
    scale_ref[0] = scale

    def put(d, e, cut, value):
        ref = sent[d - 1] if d else own_ref
        ref[e, :, cut] = value

    scale_block(xbuf.at[0], scale, acc, put, me, n, rows)
    for copy in strips:
        copy.wait()
    for turn in turns[1:]:
        for copy in turn:
            copy.wait()


def add_up(rows, *refs):
    mine_ref, acc = refs[-2:]
    for k in range(mine_ref.shape[0]):
        mine_ref[k] = add_block(refs[k], acc.at[k], rows)


def narrow(n, rows, held, x_ref, mine_ref, *refs):
    peers = refs[:n - 1]
    sent = refs[n - 1 + held:2 * n - 2 + held]
    out_ref, scale_ref, acc = refs[2 * n - 2 + held:]
    me = lax.axis_index("rows")
    total = mine_ref[0]
    for peer in peers:
        total = total + peer[0]
    scale = total / (n * x_ref.shape[-1])
    scale_ref[0] = scale

    def put(d, e, cut, value):
        ref = sent[d - 1] if d else out_ref
        ref[e, :, cut] = value

    scale_block(x_ref, scale, acc, put, me, n, rows)


def place(n, spots, *refs):
    count = len(spots)
    got, out_ref, bufs = refs[:count], refs[-3 - count], refs[-2 - count:-2]
    load_sem, store_sem = refs[-2:]
    me = lax.axis_index("rows")
    loads = [pltpu.make_async_copy(got[k], bufs[k], load_sem.at[k]) for k in range(count)]
    for copy in loads:
        copy.start()
    stores = []
    for k, (lo, d) in enumerate(spots):
        _, height, width = got[k].shape
        column = source(me, d, n) if d else me
        loads[k].wait()
        stores.append(pltpu.make_async_copy(
            bufs[k],
            out_ref.at[:, pl.ds(lo, height), pl.ds(pl.multiple_of(column * width, width), width)],
            store_sem.at[k]))
        stores[-1].start()
    for copy in stores:
        copy.wait()


def gather(owners, strip_ref, router_ref, send_sem, recv_sem):
    home = lax.axis_index("owner")
    barrier = pltpu.get_barrier_semaphore()
    for d in range(1, owners):
        pl.semaphore_signal(barrier, inc=1, device_id={"owner": lax.rem(home + d, owners)},
                            device_id_type=pl.DeviceIdType.MESH)
    pl.semaphore_wait(barrier, owners - 1)
    copies = [
        pltpu.make_async_remote_copy(
            src_ref=strip_ref, dst_ref=router_ref.at[home], send_sem=send_sem.at[d - 1],
            recv_sem=recv_sem.at[d - 1], device_id={"owner": lax.rem(home + d, owners)},
            device_id_type=pl.DeviceIdType.MESH)
        for d in range(1, owners)
    ]
    for copy in copies:
        copy.start()
    router_ref[home] = strip_ref[...]
    for copy in copies:
        copy.wait()


def cut(blocks):
    stages, done = [], 0
    for stage in STAGES:
        ends = sorted({-(-blocks * e // STAGES[-1][-1]) for e in stage} - set(range(done + 1)))
        if ends:
            stages.append([(lo, hi) for lo, hi in zip([done] + ends[:-1], ends)])
            done = ends[-1]
    return stages


def per_device(n, owners, master_down, router_weight, router_gain):
    experts, height, width = master_down.shape
    quota = height // n
    rows = block_rows(quota, experts * n)
    blocks = quota // rows
    wide = experts * n * rows
    bf16, f32 = jnp.bfloat16, jnp.float32
    x = master_down.reshape(experts, n, quota, width)
    depth, mine_e = router_weight.shape
    stages = cut(blocks)
    known = stages[0][-1][1]
    hbm = pl.BlockSpec(memory_space=pltpu.HBM)

    outs = pl.pallas_call(
        functools.partial(head, n, rows),
        out_shape=[pltpu.VMEM((experts, rows, width), bf16)] * n + [
            jax.ShapeDtypeStruct((known, 1, wide), f32),
            jax.ShapeDtypeStruct((n - 1, known, 1, wide), f32),
            jax.ShapeDtypeStruct((1, 1, wide), f32),
            jax.ShapeDtypeStruct((n, mine_e, depth), bf16),
        ],
        in_specs=[hbm, hbm, hbm],
        out_specs=[VMEM] * (n + 4),
        scratch_shapes=[
            pltpu.VMEM((known, experts, n, rows, width), f32),
            pltpu.VMEM((wide, LANES), f32),
            pltpu.VMEM((mine_e, depth), f32),
            pltpu.VMEM((1, depth), f32),
            pltpu.SemaphoreType.DMA((known,)),
            pltpu.SemaphoreType.DMA((2,)),
            pltpu.SemaphoreType.DMA((2, n - 1)),
            pltpu.SemaphoreType.DMA((2, n - 1)),
            pltpu.SemaphoreType.DMA((n - 1,)),
            pltpu.SemaphoreType.DMA((n - 1,)),
        ],
        compiler_params=pltpu.CompilerParams(
            collective_id=0, has_side_effects=True, vmem_limit_bytes=24 * MIB),
        name="head",
    )(x, router_weight.T, router_gain[None, :])
    own, mine, peers, scale0, strip = outs[n - 1:]
    peers = [peers[d] for d in range(n - 1)]
    scales = [scale0]

    def permute(arrays):
        got = []
        for d in range(1, n):
            got.append(lax.ppermute(arrays[d - 1], "rows", pairs(d, n)))
        return got

    def sums(lo, hi, after):
        step = max(k for k in (4, 3, 2, 1) if (hi - lo) % k == 0)
        return pl.pallas_call(
            functools.partial(add_up, rows),
            grid=((hi - lo) // step,),
            out_shape=jax.ShapeDtypeStruct((hi - lo, 1, wide), f32),
            in_specs=[
                pl.BlockSpec((experts, n, rows, width), lambda b, k=k: (0, 0, lo + b * step + k, 0))
                for k in range(step)
            ] + [ANY],
            out_specs=pl.BlockSpec((step, 1, wide), lambda b: (b, 0, 0)),
            scratch_shapes=[pltpu.VMEM((step, wide, LANES), f32)],
            compiler_params=pltpu.CompilerParams(vmem_limit_bytes=24 * MIB),
        )(*[x] * step, after)

    def scaled(lo, hi, base, mine, peers, out):
        part = pl.BlockSpec((1, 1, wide), lambda b: (lo - base + b, 0, 0))
        held = [] if out is None else [out]
        made = pl.pallas_call(
            functools.partial(narrow, n, rows, len(held)),
            grid=(hi - lo,),
            out_shape=[pltpu.HBM((experts, (hi - lo) * rows, width), bf16)] * (n - 1) + [
                jax.ShapeDtypeStruct((experts, quota, n * width), bf16),
                jax.ShapeDtypeStruct((hi - lo, 1, wide), f32),
            ],
            in_specs=[pl.BlockSpec((experts, n, rows, width), lambda b: (0, 0, lo + b, 0))]
            + [part] * n + [ANY] * len(held),
            out_specs=[pl.BlockSpec((experts, rows, width), lambda b: (0, b, 0))] * (n - 1) + [
                pl.BlockSpec((experts, rows, width), lambda b: (0, lo + b, lax.axis_index("rows"))),
                pl.BlockSpec((1, 1, wide), lambda b: (b, 0, 0)),
            ],
            scratch_shapes=[pltpu.VMEM((wide, LANES), f32)],
            input_output_aliases={n + 1: n - 1} if held else {},
            compiler_params=pltpu.CompilerParams(vmem_limit_bytes=16 * MIB),
        )(x, mine, *peers, *held)
        return made[:n - 1], made[n - 1], made[n]

    def placed(spots, got, out):
        count = len(got)
        return pl.pallas_call(
            functools.partial(place, n, spots),
            out_shape=jax.ShapeDtypeStruct((experts, quota, n * width), bf16),
            in_specs=[ANY] * (count + 1),
            out_specs=ANY,
            scratch_shapes=[pltpu.VMEM(a.shape, bf16) for a in got] + [
                pltpu.SemaphoreType.DMA((count,)),
                pltpu.SemaphoreType.DMA((count,)),
            ],
            input_output_aliases={count: 0},
            compiler_params=pltpu.CompilerParams(vmem_limit_bytes=24 * MIB),
        )(*got, out)

    out, got, p, base = None, [], 0, 0
    sent = list(outs[:n - 1])
    for s, stage in enumerate(stages):
        for k, (lo, hi) in enumerate(stage):
            if p:
                sent, out, part = scaled(lo, hi, base, mine, peers, out)
                scales.append(part)
            if k + 1 == len(stage) and s + 1 < len(stages):
                base, end = hi, stages[s + 1][-1][1]
                mine = sums(base, end, scales[-1])
                peers = permute([mine] * (n - 1))
            got.append(permute(sent))
            p += 1

    strips = pl.pallas_call(
        functools.partial(gather, owners),
        out_shape=jax.ShapeDtypeStruct((owners, n, mine_e, depth), bf16),
        in_specs=[VMEM],
        out_specs=VMEM,
        scratch_shapes=[pltpu.SemaphoreType.DMA((owners - 1,)), pltpu.SemaphoreType.DMA((owners - 1,))],
        compiler_params=pltpu.CompilerParams(
            collective_id=1, has_side_effects=True, vmem_limit_bytes=4 * MIB),
        name="router",
    )(strip)
    serve_router = strips.transpose(0, 2, 1, 3).reshape(owners * mine_e, n * depth).T
    held = jnp.concatenate(scales, axis=0).reshape(blocks, experts, n, rows)
    scale_down = lax.dynamic_index_in_dim(held, lax.axis_index("rows"), axis=2, keepdims=False)
    scale_down = scale_down.transpose(1, 0, 2).reshape(experts, quota)

    for p, (lo, _) in enumerate(piece for stage in stages for piece in stage):
        spots, arrays = [(lo * rows, d) for d in range(1, n)], got[p]
        if p == 0:
            spots, arrays = spots + [(0, 0)], arrays + [own]
        out = placed(tuple(spots), arrays, out)
    return out, scale_down, serve_router


def solution(mesh):
    n, owners = mesh.shape["rows"], mesh.shape["owner"]

    def body(*args):
        return per_device(n, owners, *args)

    return jax.shard_map(
        body,
        mesh=mesh,
        in_specs=(P("owner", None, "rows"), P("rows", "owner"), P("rows")),
        out_specs=(P("owner", "rows", None), P("owner", "rows"), P()),
        check_vma=False,
    )
```

```python
import functools

import jax
import jax.numpy as jnp
from jax import lax
from jax.experimental import pallas as pl
from jax.experimental.pallas import tpu as pltpu
from jax.sharding import PartitionSpec as P


LANES = 128
MIB = 1024 * 1024
ANY = pl.BlockSpec(memory_space=pl.ANY)
VMEM = pl.BlockSpec(memory_space=pltpu.VMEM)
STAGES = ((1, 3, 5), (10, 15), (24, 34, 44, 49, 50))


def block_rows(quota, count):
    fits = [r for r in (32, 16, 8) if quota % r == 0 and (count * r) % LANES == 0]
    return fits[0] if fits else quota


def partner(me, d, n):
    return me ^ d if n & (n - 1) == 0 else lax.rem(me + d, n)


def source(me, d, n):
    return me ^ d if n & (n - 1) == 0 else lax.rem(me + n - d, n)


def pairs(d, n):
    return [(i, i ^ d if n & (n - 1) == 0 else (i + d) % n) for i in range(n)]


def add_block(x, acc, rows):
    experts, n, _, width = x.shape
    for e in range(experts):
        for j in range(n):
            part = jnp.abs(x[e, j, :, :LANES])
            for g in range(1, width // LANES):
                part = part + jnp.abs(x[e, j, :, g * LANES:(g + 1) * LANES])
            at = (e * n + j) * rows
            acc[at:at + rows, :] = part
    return jnp.sum(acc[...].T, axis=0, keepdims=True)


def scale_block(x, total, acc, put, me, n, rows):
    experts, _, _, width = x.shape
    acc[...] = jnp.broadcast_to(1.0 / total, (LANES, acc.shape[0])).T
    for d in range(n):
        j = partner(me, d, n)
        for e in range(experts):
            inverse = acc[pl.ds(pl.multiple_of((e * n + j) * rows, rows), rows), :]
            for g in range(width // LANES):
                cut = slice(g * LANES, (g + 1) * LANES)
                put(d, e, cut, (x[e, j, :, cut] * inverse).astype(jnp.bfloat16))


def head(n, rows, x_ref, weight_ref, gain_ref, *refs):
    sent, (own_ref, scale_ref, strip) = refs[:n - 1], refs[n - 1:n + 2]
    (xbuf, acc, mine, peers, weight, gain, load_sem, small_sem, sum_send, sum_recv, strip_send,
     strip_recv) = refs[n + 2:]
    me = lax.axis_index("rows")
    blocks, width = xbuf.shape[0], xbuf.shape[-1]

    def load(b):
        return pltpu.make_async_copy(x_ref.at[:, :, pl.ds(b * rows, rows)], xbuf.at[b], load_sem.at[b])

    for b in range(blocks):
        load(b).start()
    smalls = [pltpu.make_async_copy(weight_ref, weight, small_sem.at[0]),
              pltpu.make_async_copy(gain_ref, gain, small_sem.at[1])]
    for copy in smalls:
        copy.start()
    barrier = pltpu.get_barrier_semaphore()
    for d in range(1, n):
        pl.semaphore_signal(barrier, inc=1, device_id={"rows": partner(me, d, n)},
                            device_id_type=pl.DeviceIdType.MESH)

    def remote(src, dst, send, recv, d):
        return pltpu.make_async_remote_copy(
            src_ref=src, dst_ref=dst, send_sem=send, recv_sem=recv,
            device_id={"rows": partner(me, d, n)}, device_id_type=pl.DeviceIdType.MESH)

    def sums(turn, lo, hi):
        return [
            remote(mine.at[pl.ds(lo, hi - lo)], peers.at[d - 1, pl.ds(lo, hi - lo)],
                   sum_send.at[turn, d - 1], sum_recv.at[turn, d - 1], d)
            for d in range(1, n)
        ]

    load(0).wait()
    mine[0] = add_block(xbuf.at[0], acc, rows)
    pl.semaphore_wait(barrier, n - 1)
    turns = [sums(0, 0, 1)] + ([sums(1, 1, blocks)] if blocks > 1 else [])
    for copy in turns[0]:
        copy.start()
    for copy in smalls:
        copy.wait()
    strip[me] = (weight[...] * gain[...]).astype(jnp.bfloat16)
    strips = [remote(strip.at[me], strip.at[me], strip_send.at[d - 1], strip_recv.at[d - 1], d)
              for d in range(1, n)]
    for copy in strips:
        copy.start()
    for b in range(1, blocks):
        load(b).wait()
        mine[b] = add_block(xbuf.at[b], acc, rows)
    for turn in turns[1:]:
        for copy in turn:
            copy.start()
    for copy in turns[0]:
        copy.wait()

    def average(b):
        total = mine[b]
        for d in range(1, n):
            total = total + peers[d - 1, b]
        scale_ref[b] = total / (n * width)

    average(0)

    def put(d, e, cut, value):
        ref = sent[d - 1] if d else own_ref
        ref[e, :, cut] = value

    scale_block(xbuf.at[0], scale_ref[0], acc, put, me, n, rows)
    for turn in turns[1:]:
        for copy in turn:
            copy.wait()
    for b in range(1, blocks):
        average(b)
    for copy in strips:
        copy.wait()


def add_up(rows, *refs):
    mine_ref, acc = refs[-2:]
    for k in range(mine_ref.shape[0]):
        mine_ref[k] = add_block(refs[k], acc.at[k], rows)


def signal_pair(me):
    pl.semaphore_signal(pltpu.get_barrier_semaphore(), inc=1, device_id={"rows": me ^ 1},
                        device_id_type=pl.DeviceIdType.MESH)


def swap_pair(me, src, dst, send_sem, recv_sem):
    pl.semaphore_wait(pltpu.get_barrier_semaphore(), 1)
    copy = pltpu.make_async_remote_copy(
        src_ref=src, dst_ref=dst, send_sem=send_sem, recv_sem=recv_sem,
        device_id={"rows": me ^ 1}, device_id_type=pl.DeviceIdType.MESH)
    copy.start()
    copy.wait()


def add_up_pair(rows, step, *refs):
    half_ref, acc, mine, theirs, send_sem, recv_sem = refs[-6:]
    me, at = lax.axis_index("rows"), pl.program_id(0)

    @pl.when(at == 0)
    def _():
        signal_pair(me)

    for k in range(step):
        mine[at * step + k] = add_block(refs[k], acc.at[k], rows)

    @pl.when(at == pl.num_programs(0) - 1)
    def _():
        swap_pair(me, mine, theirs, send_sem, recv_sem)
        part = half_ref.shape[-1]
        for core in range(2):
            @pl.when(lax.rem(me, 2) == core)
            def _():
                cut = slice(core * part, (core + 1) * part)
                half_ref[...] = mine[:, :, cut] + theirs[:, :, cut]


def finish_pair(count, half_ref, *refs):
    scale_ref, mine, theirs, send_sem, recv_sem = refs[-5:]
    me = lax.axis_index("rows")
    signal_pair(me)
    total = half_ref[...]
    for part in refs[:-5]:
        total = total + part[...]
    mine[...] = total / count
    swap_pair(me, mine, theirs, send_sem, recv_sem)
    part = half_ref.shape[-1]
    for core in range(2):
        @pl.when(lax.rem(me, 2) == core)
        def _():
            scale_ref[:, :, core * part:(core + 1) * part] = mine[...]
            scale_ref[:, :, (1 - core) * part:(2 - core) * part] = theirs[...]


def narrow(n, rows, counts, x_ref, *refs):
    held, parts = counts
    sent = refs[parts + held:parts + held + n - 1]
    out_ref, scale_ref, acc = refs[parts + held + n - 1:]
    me = lax.axis_index("rows")
    scale = refs[0][0]
    if parts > 1:
        for part in refs[1:parts]:
            scale = scale + part[0]
        scale = scale / (n * x_ref.shape[-1])
    scale_ref[0] = scale

    def put(d, e, cut, value):
        ref = sent[d - 1] if d else out_ref
        ref[e, :, cut] = value

    scale_block(x_ref, scale, acc, put, me, n, rows)


def place(n, spots, *refs):
    count = len(spots)
    got, out_ref, bufs = refs[:count], refs[-3 - count], refs[-2 - count:-2]
    load_sem, store_sem = refs[-2:]
    me = lax.axis_index("rows")
    loads = [pltpu.make_async_copy(got[k], bufs[k], load_sem.at[k]) for k in range(count)]
    for copy in loads:
        copy.start()
    stores = []
    for k, (lo, d) in enumerate(spots):
        _, height, width = got[k].shape
        column = source(me, d, n) if d else me
        loads[k].wait()
        stores.append(pltpu.make_async_copy(
            bufs[k],
            out_ref.at[:, pl.ds(lo, height), pl.ds(pl.multiple_of(column * width, width), width)],
            store_sem.at[k]))
        stores[-1].start()
    for copy in stores:
        copy.wait()


def gather(owners, strip_ref, router_ref, send_sem, recv_sem):
    home = lax.axis_index("owner")
    barrier = pltpu.get_barrier_semaphore()
    for d in range(1, owners):
        pl.semaphore_signal(barrier, inc=1, device_id={"owner": lax.rem(home + d, owners)},
                            device_id_type=pl.DeviceIdType.MESH)
    pl.semaphore_wait(barrier, owners - 1)
    copies = [
        pltpu.make_async_remote_copy(
            src_ref=strip_ref, dst_ref=router_ref.at[home], send_sem=send_sem.at[d - 1],
            recv_sem=recv_sem.at[d - 1], device_id={"owner": lax.rem(home + d, owners)},
            device_id_type=pl.DeviceIdType.MESH)
        for d in range(1, owners)
    ]
    for copy in copies:
        copy.start()
    router_ref[home] = strip_ref[...]
    for copy in copies:
        copy.wait()


def cut(blocks):
    stages, done = [], 0
    for stage in STAGES:
        ends = sorted({-(-blocks * e // STAGES[-1][-1]) for e in stage} - set(range(done + 1)))
        if ends:
            stages.append([(lo, hi) for lo, hi in zip([done] + ends[:-1], ends)])
            done = ends[-1]
    return stages


def in_pairs(s, stages, n, wide):
    return s + 2 == stages and n > 2 and n & (n - 1) == 0 and wide % (2 * LANES) == 0


def per_device(n, owners, master_down, router_weight, router_gain):
    experts, height, width = master_down.shape
    quota = height // n
    rows = block_rows(quota, experts * n)
    blocks = quota // rows
    wide = experts * n * rows
    bf16, f32 = jnp.bfloat16, jnp.float32
    x = master_down.reshape(experts, n, quota, width)
    depth, mine_e = router_weight.shape
    stages = cut(blocks)
    known = stages[0][-1][1]
    hbm = pl.BlockSpec(memory_space=pltpu.HBM)

    outs = pl.pallas_call(
        functools.partial(head, n, rows),
        out_shape=[pltpu.VMEM((experts, rows, width), bf16)] * n + [
            jax.ShapeDtypeStruct((known, 1, wide), f32),
            jax.ShapeDtypeStruct((n, mine_e, depth), bf16),
        ],
        in_specs=[hbm, hbm, hbm],
        out_specs=[VMEM] * (n + 2),
        scratch_shapes=[
            pltpu.VMEM((known, experts, n, rows, width), f32),
            pltpu.VMEM((wide, LANES), f32),
            pltpu.VMEM((known, 1, wide), f32),
            pltpu.VMEM((n - 1, known, 1, wide), f32),
            pltpu.VMEM((mine_e, depth), f32),
            pltpu.VMEM((1, depth), f32),
            pltpu.SemaphoreType.DMA((known,)),
            pltpu.SemaphoreType.DMA((2,)),
            pltpu.SemaphoreType.DMA((2, n - 1)),
            pltpu.SemaphoreType.DMA((2, n - 1)),
            pltpu.SemaphoreType.DMA((n - 1,)),
            pltpu.SemaphoreType.DMA((n - 1,)),
        ],
        compiler_params=pltpu.CompilerParams(
            collective_id=0, has_side_effects=True, vmem_limit_bytes=62 * MIB),
        name="head",
    )(x, router_weight.T, router_gain[None, :])
    own, scale, strip = outs[n - 1:]
    scales, parts, after = [scale], [scale], scale

    def move(array, d):
        return lax.ppermute(array, "rows", pairs(d, n))

    def permute(arrays):
        return [move(arrays[d - 1], d) for d in range(1, n)]

    def sums(lo, hi, after):
        step = max(k for k in (4, 3, 2, 1) if (hi - lo) % k == 0)
        return pl.pallas_call(
            functools.partial(add_up, rows),
            grid=((hi - lo) // step,),
            out_shape=jax.ShapeDtypeStruct((hi - lo, 1, wide), f32),
            in_specs=[
                pl.BlockSpec((experts, n, rows, width), lambda b, k=k: (0, 0, lo + b * step + k, 0))
                for k in range(step)
            ] + [ANY],
            out_specs=pl.BlockSpec((step, 1, wide), lambda b: (b, 0, 0)),
            scratch_shapes=[pltpu.VMEM((step, wide, LANES), f32)],
            compiler_params=pltpu.CompilerParams(vmem_limit_bytes=24 * MIB),
        )(*[x] * step, after)

    def sums_pair(lo, hi, after):
        step = max(k for k in (5, 4, 3, 2, 1) if (hi - lo) % k == 0)
        part = (hi - lo, 1, wide // 2)
        sems = [pltpu.SemaphoreType.DMA, pltpu.SemaphoreType.DMA]
        half = pl.pallas_call(
            functools.partial(add_up_pair, rows, step),
            grid=((hi - lo) // step,),
            out_shape=jax.ShapeDtypeStruct(part, f32),
            in_specs=[
                pl.BlockSpec((experts, n, rows, width), lambda b, k=k: (0, 0, lo + b * step + k, 0))
                for k in range(step)
            ] + [ANY],
            out_specs=pl.BlockSpec(part, lambda b: (0, 0, 0)),
            scratch_shapes=[
                pltpu.VMEM((step, wide, LANES), f32),
                pltpu.VMEM((hi - lo, 1, wide), f32),
                pltpu.VMEM((hi - lo, 1, wide), f32),
            ] + sems,
            compiler_params=pltpu.CompilerParams(
                collective_id=2, has_side_effects=True, vmem_limit_bytes=24 * MIB),
        )(*[x] * step, after)
        got = [move(half, d) for d in range(2, n, 2)]

        def finish():
            return pl.pallas_call(
                functools.partial(finish_pair, n * width),
                out_shape=jax.ShapeDtypeStruct((hi - lo, 1, wide), f32),
                in_specs=[VMEM] * (1 + len(got)),
                out_specs=VMEM,
                scratch_shapes=[pltpu.VMEM(part, f32), pltpu.VMEM(part, f32)] + sems,
                compiler_params=pltpu.CompilerParams(
                    collective_id=3, has_side_effects=True, vmem_limit_bytes=4 * MIB),
            )(half, *got)

        return finish

    def scaled(lo, hi, base, parts, out, limit=16):
        part = pl.BlockSpec((1, 1, wide), lambda b: (lo - base + b, 0, 0))
        held = [] if out is None else [out]
        made = pl.pallas_call(
            functools.partial(narrow, n, rows, (len(held), len(parts))),
            grid=(hi - lo,),
            out_shape=[pltpu.HBM((experts, (hi - lo) * rows, width), bf16)] * (n - 1) + [
                jax.ShapeDtypeStruct((experts, quota, n * width), bf16),
                jax.ShapeDtypeStruct((hi - lo, 1, wide), f32),
            ],
            in_specs=[pl.BlockSpec((experts, n, rows, width), lambda b: (0, 0, lo + b, 0))]
            + [part] * len(parts) + [ANY] * len(held),
            out_specs=[pl.BlockSpec((experts, rows, width), lambda b: (0, b, 0))] * (n - 1) + [
                pl.BlockSpec((experts, rows, width), lambda b: (0, lo + b, lax.axis_index("rows"))),
                pl.BlockSpec((1, 1, wide), lambda b: (b, 0, 0)),
            ],
            scratch_shapes=[pltpu.VMEM((wide, LANES), f32)],
            input_output_aliases={len(parts) + 1: n - 1} if held else {},
            compiler_params=pltpu.CompilerParams(vmem_limit_bytes=limit * MIB),
        )(x, *parts, *held)
        return made[:n - 1], made[n - 1], made[n]

    def placed(spots, got, out):
        count = len(got)
        return pl.pallas_call(
            functools.partial(place, n, spots),
            out_shape=jax.ShapeDtypeStruct((experts, quota, n * width), bf16),
            in_specs=[ANY] * (count + 1),
            out_specs=ANY,
            scratch_shapes=[pltpu.VMEM(a.shape, bf16) for a in got] + [
                pltpu.SemaphoreType.DMA((count,)),
                pltpu.SemaphoreType.DMA((count,)),
            ],
            input_output_aliases={count: 0},
            compiler_params=pltpu.CompilerParams(vmem_limit_bytes=24 * MIB),
        )(*got, out)

    out, got, p, base = None, [], 0, 0
    sent = list(outs[:n - 1])
    for s, stage in enumerate(stages):
        for k, (lo, hi) in enumerate(stage):
            if p:
                sent, out, after = scaled(lo, hi, base, parts, out, 16 if s else 62)
                if len(parts) > 1:
                    scales.append(after)
            if k + 1 == len(stage) and s + 1 < len(stages):
                base, end = hi, stages[s + 1][-1][1]
                if in_pairs(s, len(stages), n, wide):
                    finish = sums_pair(base, end, after)
                else:
                    mine = sums(base, end, after)
                    parts = [mine] + permute([mine] * (n - 1))
            got.append(permute(sent))
            p += 1
        if in_pairs(s, len(stages), n, wide):
            parts = [finish()]
            scales.append(parts[0])

    strips = pl.pallas_call(
        functools.partial(gather, owners),
        out_shape=jax.ShapeDtypeStruct((owners, n, mine_e, depth), bf16),
        in_specs=[VMEM],
        out_specs=VMEM,
        scratch_shapes=[pltpu.SemaphoreType.DMA((owners - 1,)), pltpu.SemaphoreType.DMA((owners - 1,))],
        compiler_params=pltpu.CompilerParams(
            collective_id=1, has_side_effects=True, vmem_limit_bytes=4 * MIB),
        name="router",
    )(strip)
    serve_router = strips.transpose(0, 2, 1, 3).reshape(owners * mine_e, n * depth).T
    held = jnp.concatenate(scales, axis=0).reshape(blocks, experts, n, rows)
    scale_down = lax.dynamic_index_in_dim(held, lax.axis_index("rows"), axis=2, keepdims=False)
    scale_down = scale_down.transpose(1, 0, 2).reshape(experts, quota)

    for p, (lo, _) in enumerate(piece for stage in stages for piece in stage):
        spots, arrays = [(lo * rows, d) for d in range(1, n)], got[p]
        if p == 0:
            spots, arrays = spots + [(0, 0)], arrays + [own]
        out = placed(tuple(spots), arrays, out)
    return out, scale_down, serve_router


def solution(mesh):
    n, owners = mesh.shape["rows"], mesh.shape["owner"]

    def body(*args):
        return per_device(n, owners, *args)

    return jax.shard_map(
        body,
        mesh=mesh,
        in_specs=(P("owner", None, "rows"), P("rows", "owner"), P("rows")),
        out_specs=(P("owner", "rows", None), P("owner", "rows"), P()),
        check_vma=False,
    )
```

```python
import functools

import jax
import jax.numpy as jnp
from jax import lax
from jax.experimental import pallas as pl
from jax.experimental.pallas import tpu as pltpu
from jax.sharding import PartitionSpec as P


LANES = 128
MIB = 1024 * 1024
ANY = pl.BlockSpec(memory_space=pl.ANY)
VMEM = pl.BlockSpec(memory_space=pltpu.VMEM)
STAGES = ((1, 5, 10, 15), (24, 34, 44, 49, 50))


def block_rows(quota, count):
    fits = [r for r in (32, 16, 8) if quota % r == 0 and (count * r) % LANES == 0]
    return fits[0] if fits else quota


def partner(me, d, n):
    return me ^ d if n & (n - 1) == 0 else lax.rem(me + d, n)


def source(me, d, n):
    return me ^ d if n & (n - 1) == 0 else lax.rem(me + n - d, n)


def pairs(d, n):
    return [(i, i ^ d if n & (n - 1) == 0 else (i + d) % n) for i in range(n)]


def add_block(x, acc, rows):
    experts, n, _, width = x.shape
    for e in range(experts):
        for j in range(n):
            part = jnp.abs(x[e, j, :, :LANES])
            for g in range(1, width // LANES):
                part = part + jnp.abs(x[e, j, :, g * LANES:(g + 1) * LANES])
            at = (e * n + j) * rows
            acc[at:at + rows, :] = part
    return jnp.sum(acc[...].T, axis=0, keepdims=True)


def scale_block(x, total, acc, put, me, n, rows):
    experts, _, _, width = x.shape
    acc[...] = jnp.broadcast_to(1.0 / total, (LANES, acc.shape[0])).T
    for d in range(n):
        j = partner(me, d, n)
        for e in range(experts):
            inverse = acc[pl.ds(pl.multiple_of((e * n + j) * rows, rows), rows), :]
            for g in range(width // LANES):
                cut = slice(g * LANES, (g + 1) * LANES)
                put(d, e, cut, (x[e, j, :, cut] * inverse).astype(jnp.bfloat16))


def head(n, rows, split, end, x_ref, weight_ref, gain_ref, *refs):
    sent, got = (None,) + refs[:n - 1], (None,) + refs[n - 1:2 * n - 2]
    own_ref, early_ref, scale_ref, strip = refs[2 * n - 2:2 * n + 2]
    (xbuf, nbuf, acc, mine, peers, weight, gain, load_sem, small_sem, store_sem, sum_send, sum_recv, strip_send,
     strip_recv, first_send, first_recv, early_send, early_recv) = refs[2 * n + 2:]
    me = lax.axis_index("rows")
    known, width = xbuf.shape[0], xbuf.shape[-1]

    def load(b):
        return pltpu.make_async_copy(x_ref.at[:, :, pl.ds(b * rows, rows)], xbuf.at[b], load_sem.at[b])

    for b in range(end):
        load(b).start()
    smalls = [pltpu.make_async_copy(weight_ref, weight, small_sem.at[0]),
              pltpu.make_async_copy(gain_ref, gain, small_sem.at[1])]
    for copy in smalls:
        copy.start()
    barrier = pltpu.get_barrier_semaphore()
    for d in range(1, n):
        pl.semaphore_signal(barrier, inc=1, device_id={"rows": partner(me, d, n)},
                            device_id_type=pl.DeviceIdType.MESH)

    def remote(src, dst, send, recv, d):
        return pltpu.make_async_remote_copy(
            src_ref=src, dst_ref=dst, send_sem=send, recv_sem=recv,
            device_id={"rows": partner(me, d, n)}, device_id_type=pl.DeviceIdType.MESH)

    def sums(turn, lo, hi):
        return [
            remote(mine.at[pl.ds(lo, hi - lo)], peers.at[d - 1, pl.ds(lo, hi - lo)],
                   sum_send.at[turn, d - 1], sum_recv.at[turn, d - 1], d)
            for d in range(1, n)
        ] if hi > lo else []

    def some(b):
        at = b * rows
        return pl.ds(at if isinstance(b, int) else pl.multiple_of(at, rows), rows)

    def first(d):
        return remote(nbuf.at[d, :, some(0)], got[d], first_send.at[d - 1], first_recv.at[d - 1], d)

    def early(b):
        return remote(nbuf.at[2, :, some(b)], early_ref.at[:, some(b - 1)], early_send.at[b - 1],
                      early_recv.at[b - 1], 2)

    def store(d, b):
        return pltpu.make_async_copy(nbuf.at[d, :, some(b)], sent[d].at[:, some(b - 1)], store_sem.at[d, b])

    def add(b, carry):
        load(b).wait()
        mine[b] = add_block(xbuf.at[b], acc, rows)
        return carry

    def average(lo, hi):
        if hi > lo:
            total = mine[lo:hi]
            for d in range(1, n):
                total = total + peers[d - 1, lo:hi]
            scale_ref[lo:hi] = total / (n * width)

    def scale(b):
        def put(d, e, cut, value):
            nbuf[d, e, some(b), cut] = value

        scale_block(xbuf.at[b], scale_ref[b], acc, put, me, n, rows)

    add(0, 0)
    for b in range(end, known):
        load(b).start()
    pl.semaphore_wait(barrier, n - 1)
    turns = [sums(0, 0, 1), sums(1, 1, end), sums(2, end, known)]
    for copy in turns[0]:
        copy.start()
    lax.fori_loop(1, end, add, 0)
    for copy in turns[1]:
        copy.start()
    for copy in turns[0]:
        copy.wait()
    average(0, 1)
    scale(0)
    for d in reversed(range(1, n)):
        first(d).start()
    lax.fori_loop(end, known, add, 0)
    for copy in turns[2]:
        copy.start()
    for copy in smalls:
        copy.wait()
    strip[me] = (weight[...] * gain[...]).astype(jnp.bfloat16)
    strips = [remote(strip.at[me], strip.at[me], strip_send.at[d - 1], strip_recv.at[d - 1], d)
              for d in range(1, n)]
    for copy in strips:
        copy.start()
    for copy in turns[1]:
        copy.wait()
    average(1, end)

    def step(b, carry):
        scale(b)
        for d in range(1, n):
            store(d, b).start()
        if split:
            @pl.when(lax.rem(me, 2) == 0)
            def _():
                early(b).start()
        return carry

    lax.fori_loop(1, end, step, 0)
    own = pltpu.make_async_copy(nbuf.at[0], own_ref, store_sem.at[0, 0])
    own.start()
    for copy in turns[2]:
        copy.wait()
    average(end, known)
    for copy in strips:
        copy.wait()

    def finish(b, carry):
        for d in range(1, n):
            store(d, b).wait()
        return carry

    lax.fori_loop(1, end, finish, 0)
    own.wait()
    for d in range(1, n):
        first(d).wait()
    if split:
        @pl.when(lax.rem(me, 2) == 0)
        def _():
            def arrive(b, carry):
                early(b).wait()
                return carry

            lax.fori_loop(1, end, arrive, 0)


def add_up(rows, *refs):
    mine_ref, acc = refs[-2:]
    for k in range(mine_ref.shape[0]):
        mine_ref[k] = add_block(refs[k], acc.at[k], rows)


def signal_pair(me):
    pl.semaphore_signal(pltpu.get_barrier_semaphore(), inc=1, device_id={"rows": me ^ 1},
                        device_id_type=pl.DeviceIdType.MESH)


def swap_pair(me, src, dst, send_sem, recv_sem):
    pl.semaphore_wait(pltpu.get_barrier_semaphore(), 1)
    copy = pltpu.make_async_remote_copy(
        src_ref=src, dst_ref=dst, send_sem=send_sem, recv_sem=recv_sem,
        device_id={"rows": me ^ 1}, device_id_type=pl.DeviceIdType.MESH)
    copy.start()
    copy.wait()


def add_up_pair(rows, step, *refs):
    half_ref, acc, mine, theirs, send_sem, recv_sem = refs[-6:]
    me, at = lax.axis_index("rows"), pl.program_id(0)

    @pl.when(at == 0)
    def _():
        signal_pair(me)

    for k in range(step):
        mine[at * step + k] = add_block(refs[k], acc.at[k], rows)

    @pl.when(at == pl.num_programs(0) - 1)
    def _():
        swap_pair(me, mine, theirs, send_sem, recv_sem)
        part = half_ref.shape[-1]
        for core in range(2):
            @pl.when(lax.rem(me, 2) == core)
            def _():
                cut = slice(core * part, (core + 1) * part)
                half_ref[...] = mine[:, :, cut] + theirs[:, :, cut]


def finish_pair(count, half_ref, *refs):
    scale_ref, mine, theirs, send_sem, recv_sem = refs[-5:]
    me = lax.axis_index("rows")
    signal_pair(me)
    total = half_ref[...]
    for part in refs[:-5]:
        total = total + part[...]
    mine[...] = total / count
    swap_pair(me, mine, theirs, send_sem, recv_sem)
    part = half_ref.shape[-1]
    for core in range(2):
        @pl.when(lax.rem(me, 2) == core)
        def _():
            scale_ref[:, :, core * part:(core + 1) * part] = mine[...]
            scale_ref[:, :, (1 - core) * part:(2 - core) * part] = theirs[...]


def narrow(n, rows, counts, x_ref, *refs):
    held, parts = counts
    sent = refs[parts + held:parts + held + n - 1]
    out_ref, scale_ref, acc = refs[parts + held + n - 1:]
    me = lax.axis_index("rows")
    scale = refs[0][0]
    if parts > 1:
        for part in refs[1:parts]:
            scale = scale + part[0]
        scale = scale / (n * x_ref.shape[-1])
    scale_ref[0] = scale

    def put(d, e, cut, value):
        ref = sent[d - 1] if d else out_ref
        ref[e, :, cut] = value

    scale_block(x_ref, scale, acc, put, me, n, rows)


def place(n, spots, final, *refs):
    count = len(spots)
    got = refs[:count]
    out_ref, bufs = (refs[-3], got) if final else (refs[-3 - count], refs[-2 - count:-2])
    load_sem, store_sem = refs[-2:]
    me = lax.axis_index("rows")

    def load(k):
        return pltpu.make_async_copy(got[k], bufs[k], load_sem.at[k])

    def store(k):
        lo, d, _ = spots[k]
        _, height, width = got[k].shape
        column = source(me, d, n) if d else me
        return pltpu.make_async_copy(
            bufs[k],
            out_ref.at[:, pl.ds(lo, height), pl.ds(pl.multiple_of(column * width, width), width)],
            store_sem.at[k])

    def here(k, act):
        core = spots[k][2]
        if core is None:
            act()
        else:
            pl.when(lax.rem(me, 2) == core)(act)

    def turn(k):
        if not final:
            load(k).wait()
        store(k).start()

    for k in range(0 if final else count):
        here(k, lambda: load(k).start())
    for k in range(count):
        here(k, lambda: turn(k))
    for k in range(count):
        here(k, lambda: store(k).wait())


def gather(owners, strip_ref, router_ref, send_sem, recv_sem):
    home = lax.axis_index("owner")
    barrier = pltpu.get_barrier_semaphore()
    for d in range(1, owners):
        pl.semaphore_signal(barrier, inc=1, device_id={"owner": lax.rem(home + d, owners)},
                            device_id_type=pl.DeviceIdType.MESH)
    pl.semaphore_wait(barrier, owners - 1)
    copies = [
        pltpu.make_async_remote_copy(
            src_ref=strip_ref, dst_ref=router_ref.at[home], send_sem=send_sem.at[d - 1],
            recv_sem=recv_sem.at[d - 1], device_id={"owner": lax.rem(home + d, owners)},
            device_id_type=pl.DeviceIdType.MESH)
        for d in range(1, owners)
    ]
    for copy in copies:
        copy.start()
    router_ref[home] = strip_ref[...]
    for copy in copies:
        copy.wait()


def cut(blocks):
    stages, done = [], 0
    for stage in STAGES:
        ends = sorted({-(-blocks * e // STAGES[-1][-1]) for e in stage} - set(range(done + 1)))
        if ends:
            stages.append([(lo, hi) for lo, hi in zip([done] + ends[:-1], ends)])
            done = ends[-1]
    return stages


def in_pairs(s, stages, n, wide):
    return s + 2 == stages and n > 2 and n & (n - 1) == 0 and wide % (2 * LANES) == 0


def per_device(n, owners, master_down, router_weight, router_gain):
    experts, height, width = master_down.shape
    quota = height // n
    rows = block_rows(quota, experts * n)
    blocks = quota // rows
    wide = experts * n * rows
    bf16, f32 = jnp.bfloat16, jnp.float32
    x = master_down.reshape(experts, n, quota, width)
    depth, mine_e = router_weight.shape
    stages = cut(blocks)
    known = stages[0][-1][1]
    hbm = pl.BlockSpec(memory_space=pltpu.HBM)

    end = stages[0][1][1]
    split = n > 2 and n & (n - 1) == 0
    second = ((end - 1) * rows, width)

    outs = pl.pallas_call(
        functools.partial(head, n, rows, split, end),
        out_shape=[pltpu.HBM((experts, *second), bf16)] * (n - 1) + [
            pltpu.HBM((experts, rows, width), bf16)] * (n - 1) + [
            pltpu.HBM((experts, end * rows, width), bf16),
            pltpu.HBM((experts, *(second if split else (16, LANES))), bf16),
            jax.ShapeDtypeStruct((known, 1, wide), f32),
            jax.ShapeDtypeStruct((n, mine_e, depth), bf16),
        ],
        in_specs=[hbm, hbm, hbm],
        out_specs=[ANY] * (2 * n) + [VMEM] * 2,
        scratch_shapes=[
            pltpu.VMEM((known, experts, n, rows, width), f32),
            pltpu.VMEM((n, experts, end * rows, width), bf16),
            pltpu.VMEM((wide, LANES), f32),
            pltpu.VMEM((known, 1, wide), f32),
            pltpu.VMEM((n - 1, known, 1, wide), f32),
            pltpu.VMEM((mine_e, depth), f32),
            pltpu.VMEM((1, depth), f32),
            pltpu.SemaphoreType.DMA((known,)),
            pltpu.SemaphoreType.DMA((2,)),
            pltpu.SemaphoreType.DMA((n, end)),
            pltpu.SemaphoreType.DMA((3, n - 1)),
            pltpu.SemaphoreType.DMA((3, n - 1)),
            pltpu.SemaphoreType.DMA((n - 1,)),
            pltpu.SemaphoreType.DMA((n - 1,)),
            pltpu.SemaphoreType.DMA((n - 1,)),
            pltpu.SemaphoreType.DMA((n - 1,)),
            pltpu.SemaphoreType.DMA((end,)),
            pltpu.SemaphoreType.DMA((end,)),
        ],
        compiler_params=pltpu.CompilerParams(
            collective_id=0, has_side_effects=True, vmem_limit_bytes=62 * MIB),
        name="head",
    )(x, router_weight.T, router_gain[None, :])
    own, early, scale, strip = outs[2 * n - 2:]
    scales, parts, after = [scale], [scale], scale

    def move(array, d):
        return lax.ppermute(array, "rows", pairs(d, n))

    def permute(arrays, skip=None):
        return [move(arrays[d - 1], d) for d in range(1, n) if d != skip]

    def sums(lo, hi, after):
        step = max(k for k in (4, 3, 2, 1) if (hi - lo) % k == 0)
        return pl.pallas_call(
            functools.partial(add_up, rows),
            grid=((hi - lo) // step,),
            out_shape=jax.ShapeDtypeStruct((hi - lo, 1, wide), f32),
            in_specs=[
                pl.BlockSpec((experts, n, rows, width), lambda b, k=k: (0, 0, lo + b * step + k, 0))
                for k in range(step)
            ] + [ANY],
            out_specs=pl.BlockSpec((step, 1, wide), lambda b: (b, 0, 0)),
            scratch_shapes=[pltpu.VMEM((step, wide, LANES), f32)],
            compiler_params=pltpu.CompilerParams(vmem_limit_bytes=24 * MIB),
        )(*[x] * step, after)

    def sums_pair(lo, hi, after):
        step = max(k for k in (5, 4, 3, 2, 1) if (hi - lo) % k == 0)
        part = (hi - lo, 1, wide // 2)
        sems = [pltpu.SemaphoreType.DMA, pltpu.SemaphoreType.DMA]
        half = pl.pallas_call(
            functools.partial(add_up_pair, rows, step),
            grid=((hi - lo) // step,),
            out_shape=jax.ShapeDtypeStruct(part, f32),
            in_specs=[
                pl.BlockSpec((experts, n, rows, width), lambda b, k=k: (0, 0, lo + b * step + k, 0))
                for k in range(step)
            ] + [ANY],
            out_specs=pl.BlockSpec(part, lambda b: (0, 0, 0)),
            scratch_shapes=[
                pltpu.VMEM((step, wide, LANES), f32),
                pltpu.VMEM((hi - lo, 1, wide), f32),
                pltpu.VMEM((hi - lo, 1, wide), f32),
            ] + sems,
            compiler_params=pltpu.CompilerParams(
                collective_id=2, has_side_effects=True, vmem_limit_bytes=24 * MIB),
        )(*[x] * step, after)
        got = [move(half, d) for d in range(2, n, 2)]

        def finish():
            return pl.pallas_call(
                functools.partial(finish_pair, n * width),
                out_shape=jax.ShapeDtypeStruct((hi - lo, 1, wide), f32),
                in_specs=[VMEM] * (1 + len(got)),
                out_specs=VMEM,
                scratch_shapes=[pltpu.VMEM(part, f32), pltpu.VMEM(part, f32)] + sems,
                compiler_params=pltpu.CompilerParams(
                    collective_id=3, has_side_effects=True, vmem_limit_bytes=4 * MIB),
            )(half, *got)

        return finish

    def scaled(lo, hi, base, parts, out, limit=16):
        part = pl.BlockSpec((1, 1, wide), lambda b: (lo - base + b, 0, 0))
        held = [] if out is None else [out]
        made = pl.pallas_call(
            functools.partial(narrow, n, rows, (len(held), len(parts))),
            grid=(hi - lo,),
            out_shape=[pltpu.HBM((experts, (hi - lo) * rows, width), bf16)] * (n - 1) + [
                jax.ShapeDtypeStruct((experts, quota, n * width), bf16),
                jax.ShapeDtypeStruct((hi - lo, 1, wide), f32),
            ],
            in_specs=[pl.BlockSpec((experts, n, rows, width), lambda b: (0, 0, lo + b, 0))]
            + [part] * len(parts) + [ANY] * len(held),
            out_specs=[pl.BlockSpec((experts, rows, width), lambda b: (0, b, 0))] * (n - 1) + [
                pl.BlockSpec((experts, rows, width), lambda b: (0, lo + b, lax.axis_index("rows"))),
                pl.BlockSpec((1, 1, wide), lambda b: (b, 0, 0)),
            ],
            scratch_shapes=[pltpu.VMEM((wide, LANES), f32)],
            input_output_aliases={len(parts) + 1: n - 1} if held else {},
            compiler_params=pltpu.CompilerParams(vmem_limit_bytes=limit * MIB),
        )(x, *parts, *held)
        return made[:n - 1], made[n - 1], made[n]

    def placed(spots, got, out, final):
        count = len(got)
        return pl.pallas_call(
            functools.partial(place, n, spots, final),
            out_shape=jax.ShapeDtypeStruct((experts, quota, n * width), bf16),
            in_specs=[VMEM if final else ANY] * count + [ANY],
            out_specs=ANY,
            scratch_shapes=[pltpu.VMEM(a.shape, bf16) for a in got if not final] + [
                pltpu.SemaphoreType.DMA((count,)),
                pltpu.SemaphoreType.DMA((count,)),
            ],
            input_output_aliases={count: 0},
            compiler_params=pltpu.CompilerParams(vmem_limit_bytes=24 * MIB),
        )(*got, out)

    def finish_small():
        strips = pl.pallas_call(
            functools.partial(gather, owners),
            out_shape=jax.ShapeDtypeStruct((owners, n, mine_e, depth), bf16),
            in_specs=[VMEM],
            out_specs=VMEM,
            scratch_shapes=[pltpu.SemaphoreType.DMA((owners - 1,)), pltpu.SemaphoreType.DMA((owners - 1,))],
            compiler_params=pltpu.CompilerParams(
                collective_id=1, has_side_effects=True, vmem_limit_bytes=4 * MIB),
            name="router",
        )(strip)
        serve_router = strips.transpose(0, 2, 1, 3).reshape(owners * mine_e, n * depth).T
        held = jnp.concatenate(scales, axis=0).reshape(blocks, experts, n, rows)
        scale_down = lax.dynamic_index_in_dim(held, lax.axis_index("rows"), axis=2, keepdims=False)
        scale_down = scale_down.transpose(1, 0, 2).reshape(experts, quota)
        return scale_down, serve_router

    small = None
    last = sum(len(stage) for stage in stages) - 1
    out, got, p, base = None, [list(outs[n - 1:2 * n - 2])], 0, 0
    for s, stage in enumerate(stages):
        for k, (lo, hi) in enumerate(stage):
            if p == last and len(parts) == 1:
                small = finish_small()
                parts[0], *small = lax.optimization_barrier((parts[0], *small))
            if p == 1:
                sent = outs[:n - 1]
                if split:
                    odd = lax.ppermute(sent[1], "rows", [pair for pair in pairs(2, n) if pair[0] % 2])
            if p > 1:
                sent, out, after = scaled(lo, hi, base, parts, out, 16 if s else 62)
                if len(parts) > 1:
                    scales.append(after)
            if k + 1 == len(stage) and s + 1 < len(stages):
                base, stop = hi, stages[s + 1][-1][1]
                if in_pairs(s, len(stages), n, wide):
                    finish = sums_pair(base, stop, after)
                else:
                    mine = sums(base, stop, after)
                    parts = [mine] + permute([mine] * (n - 1))
            if p:
                got.append(permute(sent, 2 if p == 1 and split else None))
            p += 1
        if in_pairs(s, len(stages), n, wide):
            parts = [finish()]
            scales.append(parts[0])

    for p, (lo, _) in enumerate(piece for stage in stages for piece in stage):
        spots, arrays = [(lo * rows, d, None) for d in range(1, n)], got[p]
        if p == 0:
            spots, arrays = spots + [(0, 0, None)], arrays + [own]
        if p == 1 and split:
            spots = [spot for spot in spots if spot[1] != 2] + [(lo * rows, 2, 0), (lo * rows, 2, 1)]
            arrays = arrays + [early, odd]
        out = placed(tuple(spots), arrays, out, p == last)
    return out, *(small or finish_small())


def solution(mesh):
    n, owners = mesh.shape["rows"], mesh.shape["owner"]

    def body(*args):
        return per_device(n, owners, *args)

    return jax.shard_map(
        body,
        mesh=mesh,
        in_specs=(P("owner", None, "rows"), P("rows", "owner"), P("rows")),
        out_specs=(P("owner", "rows", None), P("owner", "rows"), P()),
        check_vma=False,
    )
```

```python
import functools

import jax
import jax.numpy as jnp
from jax import lax
from jax.experimental import pallas as pl
from jax.experimental.pallas import tpu as pltpu
from jax.sharding import PartitionSpec as P


LANES = 128
MIB = 1024 * 1024
ANY = pl.BlockSpec(memory_space=pl.ANY)
VMEM = pl.BlockSpec(memory_space=pltpu.VMEM)
STAGES = ((1, 7, 11, 15), (27, 39, 49, 50))


def block_rows(quota, count):
    fits = [r for r in (32, 16, 8) if quota % r == 0 and (count * r) % LANES == 0]
    return fits[0] if fits else quota


def partner(me, d, n):
    return me ^ d if n & (n - 1) == 0 else lax.rem(me + d, n)


def source(me, d, n):
    return me ^ d if n & (n - 1) == 0 else lax.rem(me + n - d, n)


def pairs(d, n):
    return [(i, i ^ d if n & (n - 1) == 0 else (i + d) % n) for i in range(n)]


def add_block(x):
    experts, n, _, width = x.shape
    parts = []
    for e in range(experts):
        for j in range(n):
            part = jnp.abs(x[e, j, :, :LANES])
            for g in range(1, width // LANES):
                part = part + jnp.abs(x[e, j, :, g * LANES:(g + 1) * LANES])
            parts.append(part)
    return jnp.sum(jnp.concatenate(parts, axis=0).T, axis=0, keepdims=True)


def scale_block(x, total, acc, put, me, n, rows):
    experts, _, _, width = x.shape
    acc[...] = jnp.broadcast_to(1.0 / total, (LANES, acc.shape[0])).T
    for d in range(n):
        j = partner(me, d, n)
        for e in range(experts):
            inverse = acc[pl.ds(pl.multiple_of((e * n + j) * rows, rows), rows), :]
            inverse = jnp.concatenate([inverse] * (width // LANES), axis=1)
            put(d, e, (x[e, j] * inverse).astype(jnp.bfloat16))


def head(n, rows, split, end, x_ref, weight_ref, gain_ref, *refs):
    sent, got = (None,) + refs[:n - 1], (None,) + refs[n - 1:2 * n - 2]
    own_ref, early_ref, scale_ref, strip = refs[2 * n - 2:2 * n + 2]
    (xbuf, nbuf, acc, mine, peers, weight, gain, load_sem, small_sem, store_sem, sum_send, sum_recv, strip_send,
     strip_recv, first_send, first_recv, early_send, early_recv, raw, done, factor, raw_send, raw_recv,
     rest_send, rest_recv, done_sem) = refs[2 * n + 2:]
    me = lax.axis_index("rows")
    known, width = xbuf.shape[0], xbuf.shape[-1]

    def load(b):
        return pltpu.make_async_copy(x_ref.at[:, :, pl.ds(b * rows, rows)], xbuf.at[b], load_sem.at[b])

    for b in range(end):
        load(b).start()
    smalls = [pltpu.make_async_copy(weight_ref, weight, small_sem.at[0]),
              pltpu.make_async_copy(gain_ref, gain, small_sem.at[1])]
    for copy in smalls:
        copy.start()
    barrier = pltpu.get_barrier_semaphore()
    for d in range(1, n):
        pl.semaphore_signal(barrier, inc=1, device_id={"rows": partner(me, d, n)},
                            device_id_type=pl.DeviceIdType.MESH)

    def remote(src, dst, send, recv, d):
        return pltpu.make_async_remote_copy(
            src_ref=src, dst_ref=dst, send_sem=send, recv_sem=recv,
            device_id={"rows": partner(me, d, n)}, device_id_type=pl.DeviceIdType.MESH)

    def sums(turn, lo, hi):
        return [
            remote(mine.at[pl.ds(lo, hi - lo)], peers.at[d - 1, pl.ds(lo, hi - lo)],
                   sum_send.at[turn, d - 1], sum_recv.at[turn, d - 1], d)
            for d in range(1, n)
        ] if hi > lo else []

    def some(b):
        at = b * rows
        return pl.ds(at if isinstance(b, int) else pl.multiple_of(at, rows), rows)

    bare = raw.shape[1]
    experts = nbuf.shape[1]

    def unscaled(d):
        return remote(xbuf.at[0, 0, partner(me, d, n), pl.ds(0, bare)], raw.at[d - 1],
                      raw_send.at[d - 1], raw_recv.at[d - 1], d)

    def first(d):
        if d == 1:
            return [remote(nbuf.at[d, :, some(0)], got[d], first_send.at[d - 1], first_recv.at[d - 1], d)]
        copies = [remote(nbuf.at[d, 0, pl.ds(bare, rows - bare)], got[d].at[0, pl.ds(bare, rows - bare)],
                         first_send.at[d - 1], first_recv.at[d - 1], d)]
        if experts > 1:
            others = pl.ds(1, experts - 1)
            copies.append(remote(nbuf.at[d, others, some(0)], got[d].at[others],
                                 rest_send.at[d - 1], rest_recv.at[d - 1], d))
        return copies

    def finished(d):
        return pltpu.make_async_copy(done.at[d - 1], got[d].at[0, pl.ds(0, bare)], done_sem.at[d - 1])

    def early(b):
        return remote(nbuf.at[2, :, some(b)], early_ref.at[:, some(b - 1)], early_send.at[b - 1],
                      early_recv.at[b - 1], 2)

    def store(d, b):
        return pltpu.make_async_copy(nbuf.at[d, :, some(b)], sent[d].at[:, some(b - 1)], store_sem.at[d, b])

    def add(b, carry):
        load(b).wait()
        mine[b] = add_block(xbuf.at[b])
        return carry

    def average(lo, hi):
        if hi > lo:
            total = mine[lo:hi]
            for d in range(1, n):
                total = total + peers[d - 1, lo:hi]
            scale_ref[lo:hi] = total / (n * width)

    def scale(b):
        def put(d, e, value):
            nbuf[d, e, some(b), :] = value

        scale_block(xbuf.at[b], scale_ref[b], acc, put, me, n, rows)

    add(0, 0)
    for b in range(end, known):
        load(b).start()
    pl.semaphore_wait(barrier, n - 1)
    turns = [sums(0, 0, 1), sums(1, 1, end), sums(2, end, known)]
    for copy in turns[0]:
        copy.start()
    for d in range(2, n):
        unscaled(d).start()
    lax.fori_loop(1, end, add, 0)
    for copy in turns[1]:
        copy.start()
    for copy in turns[0]:
        copy.wait()
    average(0, 1)
    scale(0)
    factor[...] = acc[pl.ds(pl.multiple_of(me * rows, rows), bare), :]
    for d in reversed(range(1, n)):
        for copy in first(d):
            copy.start()
    lax.fori_loop(end, known, add, 0)
    for copy in turns[2]:
        copy.start()
    for copy in smalls:
        copy.wait()
    strip[me] = (weight[...] * gain[...]).astype(jnp.bfloat16)
    strips = [remote(strip.at[me], strip.at[me], strip_send.at[d - 1], strip_recv.at[d - 1], d)
              for d in range(1, n)]
    for copy in strips:
        copy.start()
    for copy in turns[1]:
        copy.wait()
    average(1, end)

    def step(b, carry):
        scale(b)
        for d in range(1, n):
            store(d, b).start()
        if split:
            @pl.when(lax.rem(me, 2) == 0)
            def _():
                early(b).start()
        return carry

    lax.fori_loop(1, end, step, 0)
    own = pltpu.make_async_copy(nbuf.at[0], own_ref, store_sem.at[0, 0])
    own.start()
    for copy in turns[2]:
        copy.wait()
    average(end, known)
    for copy in strips:
        copy.wait()

    def finish(b, carry):
        for d in range(1, n):
            store(d, b).wait()
        return carry

    lax.fori_loop(1, end, finish, 0)
    own.wait()
    for d in range(2, n):
        unscaled(d).wait()
        for g in range(width // LANES):
            cut = slice(g * LANES, (g + 1) * LANES)
            done[d - 1, :, cut] = (raw[d - 1, :, cut] * factor[...]).astype(jnp.bfloat16)
        finished(d).start()
    for d in range(2, n):
        finished(d).wait()
    for d in range(1, n):
        for copy in first(d):
            copy.wait()
    if split:
        @pl.when(lax.rem(me, 2) == 0)
        def _():
            def arrive(b, carry):
                early(b).wait()
                return carry

            lax.fori_loop(1, end, arrive, 0)


def add_up(*refs):
    mine_ref = refs[-1]
    for k in range(mine_ref.shape[0]):
        mine_ref[k] = add_block(refs[k])


def signal_pair(me):
    pl.semaphore_signal(pltpu.get_barrier_semaphore(), inc=1, device_id={"rows": me ^ 1},
                        device_id_type=pl.DeviceIdType.MESH)


def swap_pair(me, src, dst, send_sem, recv_sem):
    pl.semaphore_wait(pltpu.get_barrier_semaphore(), 1)
    copy = pltpu.make_async_remote_copy(
        src_ref=src, dst_ref=dst, send_sem=send_sem, recv_sem=recv_sem,
        device_id={"rows": me ^ 1}, device_id_type=pl.DeviceIdType.MESH)
    copy.start()
    copy.wait()


def add_up_pair(step, *refs):
    half_ref, mine, theirs, send_sem, recv_sem = refs[-5:]
    me, at = lax.axis_index("rows"), pl.program_id(0)

    @pl.when(at == 0)
    def _():
        signal_pair(me)

    for k in range(step):
        mine[at * step + k] = add_block(refs[k])

    @pl.when(at == pl.num_programs(0) - 1)
    def _():
        swap_pair(me, mine, theirs, send_sem, recv_sem)
        part = half_ref.shape[-1]
        for core in range(2):
            @pl.when(lax.rem(me, 2) == core)
            def _():
                cut = slice(core * part, (core + 1) * part)
                half_ref[...] = mine[:, :, cut] + theirs[:, :, cut]


def finish_pair(count, half_ref, *refs):
    scale_ref, mine, theirs, send_sem, recv_sem = refs[-5:]
    me = lax.axis_index("rows")
    signal_pair(me)
    total = half_ref[...]
    for part in refs[:-5]:
        total = total + part[...]
    mine[...] = total / count
    swap_pair(me, mine, theirs, send_sem, recv_sem)
    part = half_ref.shape[-1]
    for core in range(2):
        @pl.when(lax.rem(me, 2) == core)
        def _():
            scale_ref[:, :, core * part:(core + 1) * part] = mine[...]
            scale_ref[:, :, (1 - core) * part:(2 - core) * part] = theirs[...]


def narrow(n, rows, counts, x_ref, *refs):
    held, parts = counts
    sent = refs[parts + held:parts + held + n - 1]
    out_ref, scale_ref, acc = refs[parts + held + n - 1:]
    me = lax.axis_index("rows")
    scale = refs[0][0]
    if parts > 1:
        for part in refs[1:parts]:
            scale = scale + part[0]
        scale = scale / (n * x_ref.shape[-1])
    scale_ref[0] = scale

    def put(d, e, value):
        ref = sent[d - 1] if d else out_ref
        ref[e] = value

    scale_block(x_ref, scale, acc, put, me, n, rows)


def place(n, spots, final, *refs):
    count = len(spots)
    got = refs[:count]
    out_ref, bufs = (refs[-3], got) if final else (refs[-3 - count], refs[-2 - count:-2])
    load_sem, store_sem = refs[-2:]
    me = lax.axis_index("rows")

    def load(k):
        return pltpu.make_async_copy(got[k], bufs[k], load_sem.at[k])

    def store(k):
        lo, d, _ = spots[k]
        _, height, width = got[k].shape
        column = source(me, d, n) if d else me
        return pltpu.make_async_copy(
            bufs[k],
            out_ref.at[:, pl.ds(lo, height), pl.ds(pl.multiple_of(column * width, width), width)],
            store_sem.at[k])

    def here(k, act):
        core = spots[k][2]
        if core is None:
            act()
        else:
            pl.when(lax.rem(me, 2) == core)(act)

    def turn(k):
        if not final:
            load(k).wait()
        store(k).start()

    for k in range(0 if final else count):
        here(k, lambda: load(k).start())
    for k in range(count):
        here(k, lambda: turn(k))
    for k in range(count):
        here(k, lambda: store(k).wait())


def gather(owners, strip_ref, router_ref, send_sem, recv_sem):
    home = lax.axis_index("owner")
    barrier = pltpu.get_barrier_semaphore()
    for d in range(1, owners):
        pl.semaphore_signal(barrier, inc=1, device_id={"owner": lax.rem(home + d, owners)},
                            device_id_type=pl.DeviceIdType.MESH)
    pl.semaphore_wait(barrier, owners - 1)
    copies = [
        pltpu.make_async_remote_copy(
            src_ref=strip_ref, dst_ref=router_ref.at[home], send_sem=send_sem.at[d - 1],
            recv_sem=recv_sem.at[d - 1], device_id={"owner": lax.rem(home + d, owners)},
            device_id_type=pl.DeviceIdType.MESH)
        for d in range(1, owners)
    ]
    for copy in copies:
        copy.start()
    router_ref[home] = strip_ref[...]
    for copy in copies:
        copy.wait()


def cut(blocks):
    stages, done = [], 0
    for stage in STAGES:
        ends = sorted({-(-blocks * e // STAGES[-1][-1]) for e in stage} - set(range(done + 1)))
        if ends:
            stages.append([(lo, hi) for lo, hi in zip([done] + ends[:-1], ends)])
            done = ends[-1]
    return stages


def in_pairs(s, stages, n, wide):
    return s + 2 == stages and n > 2 and n & (n - 1) == 0 and wide % (2 * LANES) == 0


def per_device(n, owners, master_down, router_weight, router_gain):
    experts, height, width = master_down.shape
    quota = height // n
    rows = block_rows(quota, experts * n)
    blocks = quota // rows
    wide = experts * n * rows
    bf16, f32 = jnp.bfloat16, jnp.float32
    x = master_down.reshape(experts, n, quota, width)
    depth, mine_e = router_weight.shape
    stages = cut(blocks)
    known = stages[0][-1][1]
    hbm = pl.BlockSpec(memory_space=pltpu.HBM)

    end = stages[0][1][1]
    split = n > 2 and n & (n - 1) == 0
    second = ((end - 1) * rows, width)

    outs = pl.pallas_call(
        functools.partial(head, n, rows, split, end),
        out_shape=[pltpu.HBM((experts, *second), bf16)] * (n - 1) + [
            pltpu.HBM((experts, rows, width), bf16)] * (n - 1) + [
            pltpu.HBM((experts, end * rows, width), bf16),
            pltpu.HBM((experts, *(second if split else (16, LANES))), bf16),
            jax.ShapeDtypeStruct((known, 1, wide), f32),
            jax.ShapeDtypeStruct((n, mine_e, depth), bf16),
        ],
        in_specs=[hbm, hbm, hbm],
        out_specs=[ANY] * (2 * n) + [VMEM] * 2,
        scratch_shapes=[
            pltpu.VMEM((known, experts, n, rows, width), f32),
            pltpu.VMEM((n, experts, end * rows, width), bf16),
            pltpu.VMEM((wide, LANES), f32),
            pltpu.VMEM((known, 1, wide), f32),
            pltpu.VMEM((n - 1, known, 1, wide), f32),
            pltpu.VMEM((mine_e, depth), f32),
            pltpu.VMEM((1, depth), f32),
            pltpu.SemaphoreType.DMA((known,)),
            pltpu.SemaphoreType.DMA((2,)),
            pltpu.SemaphoreType.DMA((n, end)),
            pltpu.SemaphoreType.DMA((3, n - 1)),
            pltpu.SemaphoreType.DMA((3, n - 1)),
            pltpu.SemaphoreType.DMA((n - 1,)),
            pltpu.SemaphoreType.DMA((n - 1,)),
            pltpu.SemaphoreType.DMA((n - 1,)),
            pltpu.SemaphoreType.DMA((n - 1,)),
            pltpu.SemaphoreType.DMA((end,)),
            pltpu.SemaphoreType.DMA((end,)),
            pltpu.VMEM((n - 1, rows // 2, width), f32),
            pltpu.VMEM((n - 1, rows // 2, width), bf16),
            pltpu.VMEM((rows // 2, LANES), f32),
            pltpu.SemaphoreType.DMA((n - 1,)),
            pltpu.SemaphoreType.DMA((n - 1,)),
            pltpu.SemaphoreType.DMA((n - 1,)),
            pltpu.SemaphoreType.DMA((n - 1,)),
            pltpu.SemaphoreType.DMA((n - 1,)),
        ],
        compiler_params=pltpu.CompilerParams(
            collective_id=0, has_side_effects=True, vmem_limit_bytes=62 * MIB),
        name="head",
    )(x, router_weight.T, router_gain[None, :])
    own, early, scale, strip = outs[2 * n - 2:]
    scales, parts, after = [scale], [scale], scale

    def move(array, d):
        return lax.ppermute(array, "rows", pairs(d, n))

    def permute(arrays, skip=None):
        return [move(arrays[d - 1], d) for d in range(1, n) if d != skip]

    def sums(lo, hi, after):
        step = max(k for k in (4, 3, 2, 1) if (hi - lo) % k == 0)
        return pl.pallas_call(
            add_up,
            grid=((hi - lo) // step,),
            out_shape=jax.ShapeDtypeStruct((hi - lo, 1, wide), f32),
            in_specs=[
                pl.BlockSpec((experts, n, rows, width), lambda b, k=k: (0, 0, lo + b * step + k, 0))
                for k in range(step)
            ] + [ANY],
            out_specs=pl.BlockSpec((step, 1, wide), lambda b: (b, 0, 0)),
            compiler_params=pltpu.CompilerParams(vmem_limit_bytes=24 * MIB),
        )(*[x] * step, after)

    def sums_pair(lo, hi, after):
        step = max(k for k in (5, 4, 3, 2, 1) if (hi - lo) % k == 0)
        part = (hi - lo, 1, wide // 2)
        sems = [pltpu.SemaphoreType.DMA, pltpu.SemaphoreType.DMA]
        half = pl.pallas_call(
            functools.partial(add_up_pair, step),
            grid=((hi - lo) // step,),
            out_shape=jax.ShapeDtypeStruct(part, f32),
            in_specs=[
                pl.BlockSpec((experts, n, rows, width), lambda b, k=k: (0, 0, lo + b * step + k, 0))
                for k in range(step)
            ] + [ANY],
            out_specs=pl.BlockSpec(part, lambda b: (0, 0, 0)),
            scratch_shapes=[
                pltpu.VMEM((hi - lo, 1, wide), f32),
                pltpu.VMEM((hi - lo, 1, wide), f32),
            ] + sems,
            compiler_params=pltpu.CompilerParams(
                collective_id=2, has_side_effects=True, vmem_limit_bytes=24 * MIB),
        )(*[x] * step, after)
        got = [move(half, d) for d in range(2, n, 2)]

        def finish():
            return pl.pallas_call(
                functools.partial(finish_pair, n * width),
                out_shape=jax.ShapeDtypeStruct((hi - lo, 1, wide), f32),
                in_specs=[VMEM] * (1 + len(got)),
                out_specs=VMEM,
                scratch_shapes=[pltpu.VMEM(part, f32), pltpu.VMEM(part, f32)] + sems,
                compiler_params=pltpu.CompilerParams(
                    collective_id=3, has_side_effects=True, vmem_limit_bytes=4 * MIB),
            )(half, *got)

        return finish

    def scaled(lo, hi, base, parts, out, limit=16):
        part = pl.BlockSpec((1, 1, wide), lambda b: (lo - base + b, 0, 0))
        held = [] if out is None else [out]
        made = pl.pallas_call(
            functools.partial(narrow, n, rows, (len(held), len(parts))),
            grid=(hi - lo,),
            out_shape=[pltpu.HBM((experts, (hi - lo) * rows, width), bf16)] * (n - 1) + [
                jax.ShapeDtypeStruct((experts, quota, n * width), bf16),
                jax.ShapeDtypeStruct((hi - lo, 1, wide), f32),
            ],
            in_specs=[pl.BlockSpec((experts, n, rows, width), lambda b: (0, 0, lo + b, 0))]
            + [part] * len(parts) + [ANY] * len(held),
            out_specs=[pl.BlockSpec((experts, rows, width), lambda b: (0, b, 0))] * (n - 1) + [
                pl.BlockSpec((experts, rows, width), lambda b: (0, lo + b, lax.axis_index("rows"))),
                pl.BlockSpec((1, 1, wide), lambda b: (b, 0, 0)),
            ],
            scratch_shapes=[pltpu.VMEM((wide, LANES), f32)],
            input_output_aliases={len(parts) + 1: n - 1} if held else {},
            compiler_params=pltpu.CompilerParams(vmem_limit_bytes=limit * MIB),
        )(x, *parts, *held)
        return made[:n - 1], made[n - 1], made[n]

    def placed(spots, got, out, final):
        count = len(got)
        return pl.pallas_call(
            functools.partial(place, n, spots, final),
            out_shape=jax.ShapeDtypeStruct((experts, quota, n * width), bf16),
            in_specs=[VMEM if final else ANY] * count + [ANY],
            out_specs=ANY,
            scratch_shapes=[pltpu.VMEM(a.shape, bf16) for a in got if not final] + [
                pltpu.SemaphoreType.DMA((count,)),
                pltpu.SemaphoreType.DMA((count,)),
            ],
            input_output_aliases={count: 0},
            compiler_params=pltpu.CompilerParams(vmem_limit_bytes=24 * MIB),
        )(*got, out)

    def finish_small():
        strips = pl.pallas_call(
            functools.partial(gather, owners),
            out_shape=jax.ShapeDtypeStruct((owners, n, mine_e, depth), bf16),
            in_specs=[VMEM],
            out_specs=VMEM,
            scratch_shapes=[pltpu.SemaphoreType.DMA((owners - 1,)), pltpu.SemaphoreType.DMA((owners - 1,))],
            compiler_params=pltpu.CompilerParams(
                collective_id=1, has_side_effects=True, vmem_limit_bytes=4 * MIB),
            name="router",
        )(strip)
        serve_router = strips.transpose(0, 2, 1, 3).reshape(owners * mine_e, n * depth).T
        held = jnp.concatenate(scales, axis=0).reshape(blocks, experts, n, rows)
        scale_down = lax.dynamic_index_in_dim(held, lax.axis_index("rows"), axis=2, keepdims=False)
        scale_down = scale_down.transpose(1, 0, 2).reshape(experts, quota)
        return scale_down, serve_router

    small = None
    last = sum(len(stage) for stage in stages) - 1
    out, got, p, base = None, [list(outs[n - 1:2 * n - 2])], 0, 0
    for s, stage in enumerate(stages):
        for k, (lo, hi) in enumerate(stage):
            if p == last and len(parts) == 1:
                small = finish_small()
                parts[0], *small = lax.optimization_barrier((parts[0], *small))
            if p == 1:
                sent = outs[:n - 1]
                if split:
                    odd = lax.ppermute(sent[1], "rows", [pair for pair in pairs(2, n) if pair[0] % 2])
            if p > 1:
                sent, out, after = scaled(lo, hi, base, parts, out, 16 if s else 62)
                if len(parts) > 1:
                    scales.append(after)
            if k + 1 == len(stage) and s + 1 < len(stages):
                base, stop = hi, stages[s + 1][-1][1]
                if in_pairs(s, len(stages), n, wide):
                    finish = sums_pair(base, stop, after)
                else:
                    mine = sums(base, stop, after)
                    parts = [mine] + permute([mine] * (n - 1))
            if p:
                got.append(permute(sent, 2 if p == 1 and split else None))
            p += 1
        if in_pairs(s, len(stages), n, wide):
            parts = [finish()]
            scales.append(parts[0])

    for p, (lo, _) in enumerate(piece for stage in stages for piece in stage):
        spots, arrays = [(lo * rows, d, None) for d in range(1, n)], got[p]
        if p == 0:
            spots, arrays = spots + [(0, 0, None)], arrays + [own]
        if p == 1 and split:
            spots = [spot for spot in spots if spot[1] != 2] + [(lo * rows, 2, 0), (lo * rows, 2, 1)]
            arrays = arrays + [early, odd]
        out = placed(tuple(spots), arrays, out, p == last)
    return out, *(small or finish_small())


def solution(mesh):
    n, owners = mesh.shape["rows"], mesh.shape["owner"]

    def body(*args):
        return per_device(n, owners, *args)

    return jax.shard_map(
        body,
        mesh=mesh,
        in_specs=(P("owner", None, "rows"), P("rows", "owner"), P("rows")),
        out_specs=(P("owner", "rows", None), P("owner", "rows"), P()),
        check_vma=False,
    )
```
